128 devices in a mesh: blk: 32 (over y, x, z_lo), split: 4 (over z_hi, core).
Axes of the slice: x: 4, y: 4, z: 4 (z_hi: 2, z_lo: 2; z = z_hi * 2 + z_lo), core: 2. Of those that a mesh axis runs over, the one named last changes fastest.
Arguments:
- ratings: bfloat16 [32, 6, 4, 80, 128, 128], P('blk', None, 'split'), may hold values from -6 to 6
- user_tile: int32 [32, 6, 4, 80], P('blk', None, 'split'), may hold values from 0 to 7
- item_tile: int32 [32, 6, 4, 80], P('blk', None, 'split'), may hold values from 0 to 3
- tile_count: int32 [32, 6, 4], P('blk', None, 'split'), may hold values from 21 to 80
- user_count: int32 [32768], P('blk'), may hold values from 1 to 16
- item_count: int32 [65536], P(('blk', 'split')), may hold values from 1 to 64
- user_factors: float32 [32768, 128], P('blk'), may hold values from -0.1502602 to 0.1502602
- item_factors: float32 [65536, 128], P(('blk', 'split')), may hold values from -0.1502602 to 0.1502602
Outputs:
- users_out: float32 [32768, 128], P('blk')
- items_out: float32 [65536, 128], P(('blk', 'split'))
The draws below stay inside these ranges and needn't reach their ends.
Inputs may be any that keep to these rules, and one draw needn't show every extreme that they name: Only the first tile_count slots of a list hold ratings; the rest are ignored.
All inputs are finite; a program needn't handle non-finite values.
Results may differ from the reference program's by a relative error of at most 0.00078.
Values sent between devices are 32-bit elements; how exact they have to be, the bound alone decides.
No kernel may reach another device: no remote copies, remote signals or barrier semaphores. Data moves between devices by JAX's collectives and lax.ppermute only.
A program may use at most 128 MiB of HBM per device.

```python
import math
import jax
import jax.numpy as jnp
import numpy as np
from jax import lax

R = 128
TILE = 128
UB = 1024
PANEL = 2048
VISITS = 6
TD = 80
USERS = 32768
ITEMS = 65536
N_BLK = 32
N_SPLIT = 4


def plant(entries, stream_key, least, top_value):
    dims = entries.shape
    place = [jax.random.randint(jax.random.fold_in(stream_key, axis), (), 0, dims[axis]) for axis in range(len(dims))]
    entries = entries.at[tuple(place)].set(least)
    longest = dims.index(max(dims))
    place[longest] = (place[longest] + 1) % dims[longest]
    return entries.at[tuple(place)].set(top_value)


def level_of(stream_key, shape, cuts, least, top_value):
    level = 1.0
    for position, parts in cuts:
        heights = jax.random.uniform(jax.random.fold_in(jax.random.fold_in(stream_key, 6), position), (parts,), jnp.float32, least / len(cuts), top_value / len(cuts))
        level = level * jnp.repeat(jnp.exp(heights), shape[position] // parts).reshape((-1,) + (1,) * (len(shape) - 1 - position))
    return level


def rank_bounds(amount, skew):
    weights = [(1 << 20) // math.isqrt(rank ** skew) + 1 for rank in range(1, amount + 1)]
    deviation = 1 + sum(weights) // (1 << 30)
    return np.cumsum(np.array([max(1, weight // deviation) for weight in weights]))


def ranked_ids(stream_key, shape, amount, skew):
    grid = rank_bounds(amount, skew)
    lot = jax.random.randint(jax.random.fold_in(stream_key, 1), shape, 0, int(grid[amount - 1]))
    grade = jnp.searchsorted(jnp.asarray(grid, jnp.int32), lot, side="right")
    return jax.random.permutation(jax.random.fold_in(stream_key, 2), amount)[grade].astype(jnp.int32)


def noise(rng, extent, scale, limit, pieces=(), held_as=jnp.bfloat16):
    gain = level_of(rng, extent, pieces, -0.22, 0.18) if pieces else 1.0
    entries = jax.random.normal(rng, extent, jnp.float32) * scale * gain
    return jnp.minimum(jnp.maximum(entries, -limit), limit).astype(held_as)


def setup_inputs(seed: int = 0) -> dict:
    arg_keys = jax.random.split(jax.random.key(seed), 9)
    return {
        "ratings": noise(arg_keys[0], (N_BLK, VISITS, N_SPLIT, TD, TILE, TILE), 1.0, 6.0, ((0, 32), (2, 4))),
        "user_tile": plant(ranked_ids(arg_keys[1], (N_BLK, VISITS, N_SPLIT, TD), UB // TILE, 4), jax.random.fold_in(arg_keys[1], 3), 0, (UB // TILE) - 1).astype(jnp.int32),
        "item_tile": plant(jax.random.randint(arg_keys[2], (N_BLK, VISITS, N_SPLIT, TD), 0, PANEL // (N_SPLIT * TILE)), jax.random.fold_in(arg_keys[2], 1), 0, (PANEL // (N_SPLIT * TILE)) - 1).astype(jnp.int32),
        "tile_count": plant(jax.random.randint(arg_keys[3], (N_BLK, VISITS, N_SPLIT), TD // 4 + 1, TD + 1), jax.random.fold_in(arg_keys[3], 1), TD // 4 + 1, TD).astype(jnp.int32),
        "user_count": plant(jax.random.randint(arg_keys[4], (USERS,), 1, 17), jax.random.fold_in(arg_keys[4], 1), 1, 16).astype(jnp.int32),
        "item_count": plant(jax.random.randint(arg_keys[5], (ITEMS,), 1, 65), jax.random.fold_in(arg_keys[5], 1), 1, 64).astype(jnp.int32),
        "user_factors": jnp.clip(jax.random.uniform(arg_keys[6], (USERS, R), jnp.float32, -0.1502602, 0.1502602) * level_of(arg_keys[6], (USERS, R), ((0, 32),), -0.4, 0.0), -0.1502602, 0.1502602),
        "item_factors": jnp.clip(jax.random.uniform(arg_keys[7], (ITEMS, R), jnp.float32, -0.1502602, 0.1502602) * level_of(arg_keys[7], (ITEMS, R), ((0, 128),), -0.4, 0.0), -0.1502602, 0.1502602),
    }


step_gain = 12.0
decay_rate = 0.05

def reference(ratings, user_tile, item_tile, tile_count, user_count, item_count, user_factors, item_factors):
    part_len = PANEL // N_SPLIT
    user_tiles = UB // TILE
    item_tiles = part_len // TILE
    user_norm = TD * TILE * TILE * N_SPLIT / UB
    item_norm = TD * TILE * TILE * N_SPLIT / PANEL
    user_step = (step_gain / (user_norm * jnp.sqrt(user_count.astype(jnp.float32)))).reshape(N_BLK, UB)
    item_step = (step_gain / (item_norm * jnp.sqrt(item_count.astype(jnp.float32)))).reshape(N_BLK, N_SPLIT, part_len)
    user_rows = user_factors.reshape(N_BLK, UB, R)
    item_rows = item_factors.reshape(N_BLK, N_SPLIT, part_len, R)
    highest = lax.Precision.HIGHEST
    for visit_no in range(VISITS):
        panels = jnp.roll(item_rows, -visit_no, axis=0)
        panel_steps = jnp.roll(item_step, -visit_no, axis=0)

        def one_block(inputs):
            tile_vals, user_idx, item_idx, live_count, block_rows, block_step, panel_rows, panel_step = inputs
            user_half = block_rows.astype(jnp.bfloat16).reshape(user_tiles, TILE, R)

            def split_work(vals_s, uidx_s, iidx_s, count_s, part_rows):
                item_half = part_rows.astype(jnp.bfloat16).reshape(item_tiles, TILE, R)
                user_sel = user_half[uidx_s].astype(jnp.float32)
                item_sel = item_half[iidx_s].astype(jnp.float32)
                predicted = jnp.einsum('tur,tir->tui', user_sel, item_sel, precision=highest)
                live_mask = (jnp.arange(TD) < count_s).astype(jnp.float32)
                residual = (live_mask[:, None, None] * (vals_s.astype(jnp.float32) - predicted)).astype(jnp.bfloat16)
                res_wide = residual.astype(jnp.float32)
                grad_user_t = jnp.einsum('tui,tir->tur', res_wide, item_sel, precision=highest)
                grad_item_t = jnp.einsum('tui,tur->tir', res_wide, user_sel, precision=highest)
                grad_user = jax.ops.segment_sum(grad_user_t, uidx_s, user_tiles).reshape(UB, R)
                grad_item = jax.ops.segment_sum(grad_item_t, iidx_s, item_tiles).reshape(part_len, R)
                return (grad_user, grad_item)
            user_parts, grad_items = jax.vmap(split_work)(tile_vals, user_idx, item_idx, live_count, panel_rows)
            grad_user = lax.optimization_barrier(jnp.sum(user_parts, axis=0))
            new_block = block_rows + block_step[:, None] * (grad_user - decay_rate * block_rows)
            new_panel = panel_rows + panel_step[..., None] * (grad_items - decay_rate * panel_rows)
            return (new_block, new_panel)
        new_users, new_panels = lax.map(one_block, (ratings[:, visit_no], user_tile[:, visit_no], item_tile[:, visit_no], tile_count[:, visit_no], user_rows, user_step, panels, panel_steps))
        user_rows = new_users
        item_rows = jnp.roll(new_panels, visit_no, axis=0)
    return (user_rows.reshape(UB * N_BLK, R), item_rows.reshape(PANEL * N_BLK, R))
```

```python
import jax
import jax.numpy as jnp
from jax import lax
from jax.experimental import pallas as pl
from jax.experimental.pallas import tpu as pltpu
from jax.sharding import PartitionSpec as P

step_gain = 12.0
decay_rate = 0.05
group = 16


def from_ahead(x, axis, by):
    peers = lax.axis_size(axis)
    return lax.ppermute(x, axis, [(i, (i - by) % peers) for i in range(peers)])


def swapped(x, axis, bit):
    peers = lax.axis_size(axis)
    return lax.ppermute(x, axis, [(i, i ^ bit) for i in range(peers)])


def pair_sums(meta, ratings, visit_no, pairs):
    visits, slots, tile = ratings.shape[1], ratings.shape[3], ratings.shape[-1]
    base = visits * slots + visit_no

    def body(m, r_ref, s_ref, n_ref):
        g = pl.program_id(0)

        @pl.when(g == 0)
        def _():
            s_ref[...] = jnp.zeros_like(s_ref)
            n_ref[...] = jnp.zeros_like(n_ref)

        live = jnp.clip(m[base] - g * group, 0, group)

        def add_slot(i, carry):
            pair = m[visit_no * slots + g * group + i]
            s_ref[pair] += r_ref[0, 0, 0, i].astype(jnp.float32)
            n_ref[pl.ds(pair, 1), :] += 1.0
            return carry

        lax.fori_loop(0, live, add_slot, 0)

    return pl.pallas_call(
        body,
        grid_spec=pltpu.PrefetchScalarGridSpec(
            num_scalar_prefetch=1,
            grid=(slots // group,),
            in_specs=[
                pl.BlockSpec(
                    (1, 1, 1, group, tile, tile),
                    lambda g, m: (0, visit_no, 0, jnp.minimum(g, (m[base] - 1) // group), 0, 0),
                )
            ],
            out_specs=[
                pl.BlockSpec((pairs, tile, tile), lambda g, m: (0, 0, 0)),
                pl.BlockSpec((pairs, tile), lambda g, m: (0, 0)),
            ],
        ),
        out_shape=[
            jax.ShapeDtypeStruct((pairs, tile, tile), jnp.float32),
            jax.ShapeDtypeStruct((pairs, tile), jnp.float32),
        ],
        compiler_params=pltpu.CompilerParams(vmem_limit_bytes=16 * 2**20),
        cost_estimate=pl.CostEstimate(
            flops=slots * tile * tile * 4, transcendentals=0, bytes_accessed=slots * tile * tile * 2
        ),
        name="pair_sums",
    )(meta, ratings)


def visit(own, other, panel, sums, counts, step, first, last):
    tile = sums.shape[-1]
    half, rank = own.shape
    items = step.shape[1]
    row_tiles, col_tiles = half // tile, items // tile

    def body(own_ref, oth_ref, v_ref, s_ref, n_ref, st_ref, vout_ref, gown_ref, goth_ref):
        vt = v_ref[...].T if first else v_ref[...]
        vt16 = vt.astype(jnp.bfloat16)
        grad_t = jnp.zeros((rank, items), jnp.float32)
        for h, (u_ref, g_ref) in enumerate(((own_ref, gown_ref), (oth_ref, goth_ref))):
            u16 = u_ref[...].astype(jnp.bfloat16)
            predicted = jnp.dot(u16, vt16, preferred_element_type=jnp.float32)
            rows = []
            for a in range(row_tiles):
                cols = []
                for c in range(col_tiles):
                    pair = (h * row_tiles + a) * col_tiles + c
                    part = predicted[a * tile : (a + 1) * tile, c * tile : (c + 1) * tile]
                    cols.append((s_ref[pair] - n_ref[pair : pair + 1, :] * part).astype(jnp.bfloat16))
                rows.append(jnp.concatenate(cols, axis=1))
            error = jnp.concatenate(rows, axis=0)
            grad_t += lax.dot_general(
                u16, error, (((0,), (0,)), ((), ())), preferred_element_type=jnp.float32
            )
            g_ref[...] = lax.dot_general(
                error, vt16, (((1,), (1,)), ((), ())), preferred_element_type=jnp.float32
            )
        vnew = vt + st_ref[...] * (grad_t - decay_rate * vt)
        vout_ref[...] = vnew.T if last else vnew

    return pl.pallas_call(
        body,
        out_shape=[
            jax.ShapeDtypeStruct((items, rank) if last else (rank, items), jnp.float32),
            jax.ShapeDtypeStruct((half, rank), jnp.float32),
            jax.ShapeDtypeStruct((half, rank), jnp.float32),
        ],
        compiler_params=pltpu.CompilerParams(vmem_limit_bytes=24 * 2**20),
        cost_estimate=pl.CostEstimate(
            flops=3 * 2 * 2 * half * items * rank, transcendentals=0, bytes_accessed=4 * 2**20
        ),
        name="visit",
    )(own, other, panel, sums, counts, step)


def per_device(
    ratings, user_tile, item_tile, tile_count, user_count, item_count, user_factors, item_factors
):
    visit_total = ratings.shape[1]
    slot_total = ratings.shape[3]
    tile_len = ratings.shape[-1]
    split_count = lax.axis_size("split")
    user_total, rank = user_factors.shape
    item_total = item_factors.shape[0]
    half = user_total // 2
    user_tiles, item_tiles = user_total // tile_len, item_total // tile_len
    pairs = user_tiles * item_tiles
    side = lax.axis_index("split") % 2

    place = (user_tile.reshape(-1) + side * (user_tiles // 2)) % user_tiles
    meta = jnp.concatenate([place * item_tiles + item_tile.reshape(-1), tile_count.reshape(-1)])

    user_norm = slot_total * tile_len * tile_len * split_count / user_total
    item_norm = slot_total * tile_len * tile_len / item_total
    item_step = (step_gain / (item_norm * jnp.sqrt(item_count.astype(jnp.float32))))[None, :]
    own_count = lax.dynamic_slice_in_dim(user_count, side * half, half, 0)
    own_step = step_gain / (user_norm * jnp.sqrt(own_count.astype(jnp.float32)))
    own_step = lax.optimization_barrier(jnp.broadcast_to(own_step[:, None], (half, rank)))

    one = from_ahead(item_step, "blk", 1)
    both = jnp.concatenate([item_step, one])
    two, four = from_ahead(both, "blk", 2), from_ahead(both, "blk", 4)
    steps = [item_step, one, two[:1], two[1:], four[:1], four[1:]]

    own = lax.dynamic_slice_in_dim(user_factors, side * half, half, 0)
    other = lax.dynamic_slice_in_dim(user_factors, (1 - side) * half, half, 0)
    panel = item_factors
    for visit_no in range(visit_total):
        first, last = visit_no == 0, visit_no == visit_total - 1
        sums, counts = pair_sums(meta, ratings, visit_no, pairs)
        panel, grad_own, grad_other = visit(
            own, other, panel, sums, counts, steps[visit_no], first, last
        )
        panel = from_ahead(panel, "blk", 1 - visit_total if last else 1)
        chip_grad = grad_own + swapped(grad_other, "split", 1)
        grad = chip_grad + swapped(chip_grad, "split", 2)
        own = own + own_step * (grad - decay_rate * own)
        other = swapped(own, "split", 1)
    low = side == 0
    users = jnp.concatenate([jnp.where(low, own, other), jnp.where(low, other, own)])
    return (users, panel)


def solution(mesh):
    return jax.shard_map(
        per_device,
        mesh=mesh,
        in_specs=(
            P("blk", None, "split", None, None, None),
            P("blk", None, "split", None),
            P("blk", None, "split", None),
            P("blk", None, "split"),
            P("blk"),
            P(("blk", "split")),
            P("blk", None),
            P(("blk", "split"), None),
        ),
        out_specs=(P("blk", None), P(("blk", "split"), None)),
        check_vma=False,
    )
```

```python
import jax
import jax.numpy as jnp
from jax import lax
from jax.experimental import pallas as pl
from jax.experimental.pallas import tpu as pltpu
from jax.sharding import PartitionSpec as P


step_gain = 12.0
decay_rate = 0.05
group = 8
f32, bf16 = jnp.float32, jnp.bfloat16
hbm = pl.BlockSpec(memory_space=pltpu.HBM)
smem = pl.BlockSpec(memory_space=pltpu.SMEM)
vmem = pl.BlockSpec(memory_space=pltpu.VMEM)


def from_ahead(x, axis, by):
    peers = lax.axis_size(axis)
    return lax.ppermute(x, axis, [(i, (i - by) % peers) for i in range(peers)])


def swapped(x, axis, bit):
    peers = lax.axis_size(axis)
    return lax.ppermute(x, axis, [(i, i ^ bit) for i in range(peers)])


class Sizes:
    def __init__(self, ratings, user_factors, item_factors):
        self.visits, self.slots, self.tile = ratings.shape[1], ratings.shape[3], ratings.shape[-1]
        self.users, self.rank = user_factors.shape
        self.items = item_factors.shape[0]
        self.half = self.users // 2
        self.row_tiles, self.col_tiles = self.half // self.tile, self.items // self.tile
        self.half_pairs = self.row_tiles * self.col_tiles
        self.sum_rows = self.half_pairs * self.tile + self.half_pairs
        self.panel_rows = self.items + -(-self.col_tiles // 8) * 8


def live_copies(z, visit_no, r_hbm, buf, sems):
    return [
        pltpu.make_async_copy(
            r_hbm.at[0, visit_no, 0, pl.ds(g * group, group)],
            buf.at[pl.ds(g * group, group)],
            sems.at[g],
        )
        for g in range(z.slots // group)
    ]


def start_live(live, copies):
    for g, copy in enumerate(copies):
        @pl.when(g * group < live)
        def _():
            copy.start()


def add_live(z, visit_no, side, live, copies, ut, it, buf, own_ref, oth_ref):
    own_ref[...] = jnp.zeros_like(own_ref)
    oth_ref[...] = jnp.zeros_like(oth_ref)
    count_row = z.half_pairs * z.tile

    def add_slot(t, carry):
        user = lax.rem(ut[0, visit_no, 0, t] + side * z.row_tiles, 2 * z.row_tiles)
        pair = user * z.col_tiles + it[0, visit_no, 0, t]

        def add_to(ref, pair):
            row = pl.multiple_of(pair * z.tile, z.tile)
            ref[pl.ds(row, z.tile), :] += buf[t].astype(f32)
            ref[pl.ds(count_row + pair, 1), :] += 1.0

        @pl.when(pair < z.half_pairs)
        def _():
            add_to(own_ref, pair)

        @pl.when(pair >= z.half_pairs)
        def _():
            add_to(oth_ref, pair - z.half_pairs)

        return carry

    for g, copy in enumerate(copies):
        @pl.when(g * group < live)
        def _():
            copy.wait()
            lax.fori_loop(g * group, jnp.minimum(live, (g + 1) * group), add_slot, 0)


def pair_sums(z, visit_no, side, tiles, ratings, after, user_count=None, split_count=None):
    with_steps = user_count is not None

    def body(side_ref, ut, it, cnt, r_hbm, _, *refs):
        live = cnt[visit_no]
        if with_steps:
            count_ref, own_ref, oth_ref, step_ref, buf, sems = refs
        else:
            own_ref, oth_ref, buf, sems = refs
        copies = live_copies(z, visit_no, r_hbm, buf, sems)
        start_live(live, copies)
        if with_steps:
            user_norm = z.slots * z.tile * z.tile * split_count / z.users
            for a in range(z.row_tiles):
                count = count_ref[pl.ds(side_ref[0] * z.row_tiles + a, 1), :].astype(f32)
                step = step_gain / (user_norm * jnp.sqrt(count))
                rows = jnp.broadcast_to(step, (z.tile, z.tile)).T
                step_ref[a * z.tile : (a + 1) * z.tile, :] = rows
        add_live(z, visit_no, side_ref[0], live, copies, ut, it, buf, own_ref, oth_ref)

    out = jax.ShapeDtypeStruct((z.sum_rows, z.tile), f32)
    return pl.pallas_call(
        body,
        in_specs=[smem] * 4 + [hbm, pl.BlockSpec(memory_space=pl.ANY)] + [vmem] * with_steps,
        out_specs=[vmem] * (2 + with_steps),
        out_shape=[out, out] + [jax.ShapeDtypeStruct((z.half, z.rank), f32)] * with_steps,
        scratch_shapes=[
            pltpu.VMEM((z.slots, z.tile, z.tile), bf16),
            pltpu.SemaphoreType.DMA((z.slots // group,)),
        ],
        compiler_params=pltpu.CompilerParams(vmem_limit_bytes=16 * 2**20),
        cost_estimate=pl.CostEstimate(
            flops=z.slots * z.tile * z.tile * 4,
            transcendentals=0,
            bytes_accessed=z.slots * z.tile * z.tile * 2,
        ),
        name="pair_sums",
    )(side, *tiles, ratings, after, *([user_count.reshape(-1, z.tile)] if with_steps else []))


def errors(z, u16, vt16, s_ref):
    predicted = jnp.dot(u16, vt16, preferred_element_type=f32)
    count_row = z.half_pairs * z.tile
    rows = []
    for a in range(z.row_tiles):
        cols = []
        for c in range(z.col_tiles):
            pair = a * z.col_tiles + c
            part = predicted[a * z.tile : (a + 1) * z.tile, c * z.tile : (c + 1) * z.tile]
            sums = s_ref[pair * z.tile : (pair + 1) * z.tile, :]
            count = s_ref[count_row + pair : count_row + pair + 1, :]
            cols.append((sums - count * part).astype(bf16))
        rows.append(jnp.concatenate(cols, axis=1))
    return jnp.concatenate(rows, axis=0)


def user_grad(error, vt16):
    return lax.dot_general(error, vt16, (((1,), (1,)), ((), ())), preferred_element_type=f32)


def item_grad(u16, error):
    return lax.dot_general(u16, error, (((0,), (0,)), ((), ())), preferred_element_type=f32)


def read_panel(z, m_ref):
    blocks = [m_ref[c * z.tile : (c + 1) * z.tile, :] for c in range(z.col_tiles)]
    return jnp.concatenate(blocks, axis=1)


def read_steps(z, m_ref):
    return jnp.concatenate([m_ref[z.items + c : z.items + c + 1, :] for c in range(z.col_tiles)], axis=1)


def write_panel(z, m_ref, vt, step):
    m_ref[z.items :, :] = jnp.zeros((z.panel_rows - z.items, z.tile), f32)
    for c in range(z.col_tiles):
        cols = slice(c * z.tile, (c + 1) * z.tile)
        m_ref[c * z.tile : (c + 1) * z.tile, :] = vt[:, cols]
        m_ref[z.items + c : z.items + c + 1, :] = step[:, cols]


def updated(vt, step, grad_t):
    return vt + step * (grad_t - decay_rate * vt)


def visit_cost(z, quarters):
    flops = 2 * z.half * z.items * z.rank * quarters
    return pl.CostEstimate(flops=flops, transcendentals=0, bytes_accessed=4 * 2**20)


def first_visit(z, side, tiles, ratings, user_factors, item_factors, item_count):
    def body(
        side_ref, ut, it, cnt, r_hbm, u_hbm, v_hbm, ic_ref,
        m_ref, gown_ref, goth_ref, own_ref,
        buf, s_own, s_oth, oth_ref, v_ref, sems, fsems,
    ):
        side = side_ref[0]
        live = cnt[0]
        copies = live_copies(z, 0, r_hbm, buf, sems)
        start_live(live, copies)
        own_at = pl.multiple_of(side * z.half, z.half)
        oth_at = pl.multiple_of((1 - side) * z.half, z.half)
        factors = [
            pltpu.make_async_copy(u_hbm.at[pl.ds(own_at, z.half)], own_ref, fsems.at[0]),
            pltpu.make_async_copy(u_hbm.at[pl.ds(oth_at, z.half)], oth_ref, fsems.at[1]),
            pltpu.make_async_copy(v_hbm, v_ref, fsems.at[2]),
        ]
        for copy in factors:
            copy.start()
        add_live(z, 0, side, live, copies, ut, it, buf, s_own, s_oth)
        for copy in factors:
            copy.wait()
        item_norm = z.slots * z.tile * z.tile / z.items
        step = step_gain / (item_norm * jnp.sqrt(ic_ref[...].astype(f32)))
        step = jnp.concatenate([step[c : c + 1, :] for c in range(z.col_tiles)], axis=1)
        vt = jnp.concatenate(
            [v_ref[c * z.tile : (c + 1) * z.tile, :].T for c in range(z.col_tiles)], axis=1
        )
        vt16 = vt.astype(bf16)
        grad_t = jnp.zeros((z.rank, z.items), f32)
        for u_ref, s_ref, g_ref in ((own_ref, s_own, gown_ref), (oth_ref, s_oth, goth_ref)):
            u16 = u_ref[...].astype(bf16)
            error = errors(z, u16, vt16, s_ref)
            grad_t += item_grad(u16, error)
            g_ref[...] = user_grad(error, vt16)
        write_panel(z, m_ref, updated(vt, step, grad_t), step)

    half = jax.ShapeDtypeStruct((z.half, z.rank), f32)
    return pl.pallas_call(
        body,
        in_specs=[smem, smem, smem, smem, hbm, hbm, hbm, vmem],
        out_specs=[vmem] * 4,
        out_shape=[jax.ShapeDtypeStruct((z.panel_rows, z.tile), f32), half, half, half],
        scratch_shapes=[
            pltpu.VMEM((z.slots, z.tile, z.tile), bf16),
            pltpu.VMEM((z.sum_rows, z.tile), f32),
            pltpu.VMEM((z.sum_rows, z.tile), f32),
            pltpu.VMEM((z.half, z.rank), f32),
            pltpu.VMEM((z.items, z.rank), f32),
            pltpu.SemaphoreType.DMA((z.slots // group,)),
            pltpu.SemaphoreType.DMA((3,)),
        ],
        compiler_params=pltpu.CompilerParams(vmem_limit_bytes=28 * 2**20),
        cost_estimate=visit_cost(z, 6),
        name="first_visit",
    )(side, *tiles, ratings, user_factors, item_factors, item_count)


def visit(z, own, other, panel, partner_panel, s_own, s_oth, s_partner, last):
    def body(own_ref, oth_ref, m_ref, x_ref, so_ref, st_ref, sx_ref, mout_ref, g_ref):
        vt = read_panel(z, m_ref)
        step = read_steps(z, m_ref)
        vt16 = vt.astype(bf16)
        own16 = own_ref[...].astype(bf16)
        oth16 = oth_ref[...].astype(bf16)
        error = errors(z, own16, vt16, so_ref)
        grad_t = item_grad(own16, error)
        grad = user_grad(error, vt16)
        grad_t += item_grad(oth16, errors(z, oth16, vt16, st_ref))
        vnew = updated(vt, step, grad_t)
        if last:
            for c in range(z.col_tiles):
                cols = slice(c * z.tile, (c + 1) * z.tile)
                mout_ref[c * z.tile : (c + 1) * z.tile, :] = vnew[:, cols].T
        else:
            write_panel(z, mout_ref, vnew, step)
        xt16 = read_panel(z, x_ref).astype(bf16)
        g_ref[...] = grad + user_grad(errors(z, own16, xt16, sx_ref), xt16)

    rows = z.items if last else z.panel_rows
    return pl.pallas_call(
        body,
        in_specs=[vmem] * 7,
        out_specs=[vmem] * 2,
        out_shape=[
            jax.ShapeDtypeStruct((rows, z.tile), f32),
            jax.ShapeDtypeStruct((z.half, z.rank), f32),
        ],
        compiler_params=pltpu.CompilerParams(vmem_limit_bytes=24 * 2**20),
        cost_estimate=visit_cost(z, 7),
        name="visit",
    )(own, other, panel, partner_panel, s_own, s_oth, s_partner)


def outputs(z, side, own, other, panel):
    def body(side_ref, own_ref, oth_ref, v_ref, u_hbm, v_hbm, sems):
        side = side_ref[0]
        own_at = pl.multiple_of(side * z.half, z.half)
        oth_at = pl.multiple_of((1 - side) * z.half, z.half)
        copies = [
            pltpu.make_async_copy(own_ref, u_hbm.at[pl.ds(own_at, z.half)], sems.at[0]),
            pltpu.make_async_copy(oth_ref, u_hbm.at[pl.ds(oth_at, z.half)], sems.at[1]),
            pltpu.make_async_copy(v_ref, v_hbm, sems.at[2]),
        ]
        for copy in copies:
            copy.start()
        for copy in copies:
            copy.wait()

    return pl.pallas_call(
        body,
        in_specs=[smem, vmem, vmem, vmem],
        out_specs=[hbm, hbm],
        out_shape=[
            jax.ShapeDtypeStruct((z.users, z.rank), f32),
            jax.ShapeDtypeStruct((z.items, z.rank), f32),
        ],
        scratch_shapes=[pltpu.SemaphoreType.DMA((3,))],
        compiler_params=pltpu.CompilerParams(vmem_limit_bytes=8 * 2**20),
        name="outputs",
    )(side, own, other, panel)


def per_device(
    ratings, user_tile, item_tile, tile_count, user_count, item_count, user_factors, item_factors
):
    z = Sizes(ratings, user_factors, item_factors)
    core = lax.axis_index("split") % 2
    side = core.astype(jnp.int32).reshape(1)
    tiles = (user_tile, item_tile, tile_count.reshape(-1))
    ratings, user_factors, item_factors = (
        pltpu.with_memory_space_constraint(x, pltpu.HBM)
        for x in (ratings, user_factors, item_factors)
    )

    panel, grad, grad_other, own = first_visit(
        z, side, tiles, ratings, user_factors, item_factors, item_count.reshape(-1, z.tile)
    )
    for visit_no in range(z.visits):
        last = visit_no == z.visits - 1
        if visit_no > 0:
            panel, grad = visit(z, own, other, panel, partner_panel, s_own, s_oth, s_partner, last)
        panel = from_ahead(panel, "blk", 1 - z.visits if last else 1)
        if not last:
            if visit_no == 0:
                s_own, s_oth, own_step = pair_sums(
                    z, 1, side, tiles, ratings, grad, user_count, lax.axis_size("split")
                )
            else:
                s_own, s_oth = pair_sums(z, visit_no + 1, side, tiles, ratings, grad)
            s_partner = swapped(s_oth, "split", 1)
        if visit_no == 0:
            grad = grad + swapped(grad_other, "split", 1)
        crossed = swapped(grad, "split", 2)
        grad = grad + crossed
        own = own + own_step * (grad - decay_rate * own)
        other = swapped(own, "split", 1)
        if not last:
            partner_panel = swapped(panel, "split", 1)
    return outputs(z, side, own, other, panel)


def solution(mesh):
    return jax.shard_map(
        per_device,
        mesh=mesh,
        in_specs=(
            P("blk", None, "split", None, None, None),
            P("blk", None, "split", None),
            P("blk", None, "split", None),
            P("blk", None, "split"),
            P("blk"),
            P(("blk", "split")),
            P("blk", None),
            P(("blk", "split"), None),
        ),
        out_specs=(P("blk", None), P(("blk", "split"), None)),
        check_vma=False,
    )
```

```python
import jax
import jax.numpy as jnp
from jax import lax
from jax.experimental import pallas as pl
from jax.experimental.pallas import tpu as pltpu
from jax.sharding import PartitionSpec as P


step_gain = 12.0
decay_rate = 0.05
group = 8
f32, bf16 = jnp.float32, jnp.bfloat16
hbm = pl.BlockSpec(memory_space=pltpu.HBM)
smem = pl.BlockSpec(memory_space=pltpu.SMEM)
vmem = pl.BlockSpec(memory_space=pltpu.VMEM)


def from_ahead(x, axis, by):
    peers = lax.axis_size(axis)
    return lax.ppermute(x, axis, [(i, (i - by) % peers) for i in range(peers)])


def swapped(x, axis, bit):
    peers = lax.axis_size(axis)
    return lax.ppermute(x, axis, [(i, i ^ bit) for i in range(peers)])


class Sizes:
    def __init__(self, ratings, user_factors, item_factors):
        self.visits, self.slots, self.tile = ratings.shape[1], ratings.shape[3], ratings.shape[-1]
        self.users, self.rank = user_factors.shape
        self.items = item_factors.shape[0]
        self.half = self.users // 2
        self.row_tiles, self.col_tiles = self.half // self.tile, self.items // self.tile
        self.half_pairs = self.row_tiles * self.col_tiles
        self.sum_rows = self.half_pairs * self.tile + self.half_pairs
        self.panel_rows = self.items + -(-self.col_tiles // 8) * 8


def group_copy(visit_no, r_hbm, buf, sems, g):
    slots = pl.ds(g * group, group)
    return pltpu.make_async_copy(r_hbm.at[0, visit_no, 0, slots], buf.at[slots], sems.at[g])


def start_live(z, visit_no, live, r_hbm, buf, sems):
    for g in range(z.slots // group):
        @pl.when(g * group < live)
        def _():
            group_copy(visit_no, r_hbm, buf, sems, g).start()


def add_live(z, visit_no, side, live, ut, it, r_hbm, buf, sems, sum_ref):
    sum_ref[...] = jnp.zeros_like(sum_ref)
    count_row = z.half_pairs * z.tile

    def add_slot(t):
        user = ut[0, visit_no, 0, t] + side * z.row_tiles
        user = jnp.where(user >= 2 * z.row_tiles, user - 2 * z.row_tiles, user)
        half = jnp.where(user >= z.row_tiles, 1, 0)
        pair = (user - half * z.row_tiles) * z.col_tiles + it[0, visit_no, 0, t]
        row = pl.multiple_of(half * z.sum_rows + pair * z.tile, 8)
        sum_ref[pl.ds(row, z.tile), :] += buf[t].astype(f32)
        sum_ref[pl.ds(half * z.sum_rows + count_row + pair, 1), :] += 1.0

    def add_group(g, carry):
        group_copy(visit_no, r_hbm, buf, sems, g).wait()
        for i in range(group):
            add_slot(g * group + i)
        return carry

    def add_one(t, carry):
        add_slot(t)
        return carry

    full = live // group
    lax.fori_loop(0, full, add_group, 0)

    @pl.when(full * group < live)
    def _():
        group_copy(visit_no, r_hbm, buf, sems, full).wait()
        lax.fori_loop(full * group, live, add_one, 0)


def pair_sums(z, visit_no, side, tiles, ratings, after, user_count=None, split_count=None):
    with_steps = user_count is not None

    def body(side_ref, ut, it, cnt, r_hbm, _, *refs):
        live = cnt[visit_no]
        if with_steps:
            count_ref, own_ref, oth_ref, step_ref, buf, sum_ref, sems = refs
        else:
            own_ref, oth_ref, buf, sum_ref, sems = refs
        start_live(z, visit_no, live, r_hbm, buf, sems)
        if with_steps:
            user_norm = z.slots * z.tile * z.tile * split_count / z.users
            for a in range(z.row_tiles):
                count = count_ref[pl.ds(side_ref[0] * z.row_tiles + a, 1), :].astype(f32)
                step = step_gain / (user_norm * jnp.sqrt(count))
                rows = jnp.broadcast_to(step, (z.tile, z.tile)).T
                step_ref[a * z.tile : (a + 1) * z.tile, :] = rows
        add_live(z, visit_no, side_ref[0], live, ut, it, r_hbm, buf, sems, sum_ref)
        own_ref[...] = sum_ref[: z.sum_rows, :]
        oth_ref[...] = sum_ref[z.sum_rows :, :]

    out = jax.ShapeDtypeStruct((z.sum_rows, z.tile), f32)
    return pl.pallas_call(
        body,
        in_specs=[smem] * 4 + [hbm, pl.BlockSpec(memory_space=pl.ANY)] + [vmem] * with_steps,
        out_specs=[vmem] * (2 + with_steps),
        out_shape=[out, out] + [jax.ShapeDtypeStruct((z.half, z.rank), f32)] * with_steps,
        scratch_shapes=[
            pltpu.VMEM((z.slots, z.tile, z.tile), bf16),
            pltpu.VMEM((2 * z.sum_rows, z.tile), f32),
            pltpu.SemaphoreType.DMA((z.slots // group,)),
        ],
        compiler_params=pltpu.CompilerParams(vmem_limit_bytes=16 * 2**20),
        cost_estimate=pl.CostEstimate(
            flops=z.slots * z.tile * z.tile * 4,
            transcendentals=0,
            bytes_accessed=z.slots * z.tile * z.tile * 2,
        ),
        name="pair_sums",
    )(side, *tiles, ratings, after, *([user_count.reshape(-1, z.tile)] if with_steps else []))


def errors(z, u16, vt16, s_ref, base=0):
    predicted = jnp.dot(u16, vt16, preferred_element_type=f32)
    count_row = base + z.half_pairs * z.tile
    rows = []
    for a in range(z.row_tiles):
        cols = []
        for c in range(z.col_tiles):
            pair = a * z.col_tiles + c
            part = predicted[a * z.tile : (a + 1) * z.tile, c * z.tile : (c + 1) * z.tile]
            sums = s_ref[base + pair * z.tile : base + (pair + 1) * z.tile, :]
            count = s_ref[count_row + pair : count_row + pair + 1, :]
            cols.append((sums - count * part).astype(bf16))
        rows.append(jnp.concatenate(cols, axis=1))
    return jnp.concatenate(rows, axis=0)


def user_grad(error, vt16):
    return lax.dot_general(error, vt16, (((1,), (1,)), ((), ())), preferred_element_type=f32)


def item_grad(u16, error):
    return lax.dot_general(u16, error, (((0,), (0,)), ((), ())), preferred_element_type=f32)


def read_panel(z, m_ref):
    blocks = [m_ref[c * z.tile : (c + 1) * z.tile, :] for c in range(z.col_tiles)]
    return jnp.concatenate(blocks, axis=1)


def read_steps(z, m_ref):
    return jnp.concatenate([m_ref[z.items + c : z.items + c + 1, :] for c in range(z.col_tiles)], axis=1)


def write_panel(z, m_ref, vt, step):
    m_ref[z.items :, :] = jnp.zeros((z.panel_rows - z.items, z.tile), f32)
    for c in range(z.col_tiles):
        cols = slice(c * z.tile, (c + 1) * z.tile)
        m_ref[c * z.tile : (c + 1) * z.tile, :] = vt[:, cols]
        m_ref[z.items + c : z.items + c + 1, :] = step[:, cols]


def updated(vt, step, grad_t):
    return vt + step * (grad_t - decay_rate * vt)


def visit_cost(z, quarters):
    flops = 2 * z.half * z.items * z.rank * quarters
    return pl.CostEstimate(flops=flops, transcendentals=0, bytes_accessed=4 * 2**20)


def first_visit(z, side, tiles, ratings, user_factors, item_factors, item_count):
    def body(
        side_ref, ut_hbm, it_hbm, cnt_hbm, r_hbm, u_hbm, v_hbm, ic_hbm,
        m_ref, gown_ref, goth_ref, own_ref,
        buf, sum_ref, oth_ref, v_ref, ic_ref, ut, it, cnt, sems, fsems, isems,
    ):
        side = side_ref[0]
        indices = [
            pltpu.make_async_copy(src, dst, isems.at[i])
            for i, (src, dst) in enumerate(((cnt_hbm, cnt), (ut_hbm, ut), (it_hbm, it)))
        ]
        for copy in indices:
            copy.start()
        indices[0].wait()
        live = cnt[0]
        start_live(z, 0, live, r_hbm, buf, sems)
        own_at = pl.multiple_of(side * z.half, z.half)
        oth_at = pl.multiple_of((1 - side) * z.half, z.half)
        factors = [
            pltpu.make_async_copy(u_hbm.at[pl.ds(own_at, z.half)], own_ref, fsems.at[0]),
            pltpu.make_async_copy(u_hbm.at[pl.ds(oth_at, z.half)], oth_ref, fsems.at[1]),
            pltpu.make_async_copy(v_hbm, v_ref, fsems.at[2]),
            pltpu.make_async_copy(ic_hbm, ic_ref, fsems.at[3]),
        ]
        for copy in factors:
            copy.start()
        for copy in indices[1:]:
            copy.wait()
        add_live(z, 0, side, live, ut, it, r_hbm, buf, sems, sum_ref)
        for copy in factors:
            copy.wait()
        item_norm = z.slots * z.tile * z.tile / z.items
        step = step_gain / (item_norm * jnp.sqrt(ic_ref[...].astype(f32)))
        step = jnp.concatenate([step[c : c + 1, :] for c in range(z.col_tiles)], axis=1)
        vt = jnp.concatenate(
            [v_ref[c * z.tile : (c + 1) * z.tile, :].T for c in range(z.col_tiles)], axis=1
        )
        vt16 = vt.astype(bf16)
        grad_t = jnp.zeros((z.rank, z.items), f32)
        for h, (u_ref, g_ref) in enumerate(((own_ref, gown_ref), (oth_ref, goth_ref))):
            u16 = u_ref[...].astype(bf16)
            error = errors(z, u16, vt16, sum_ref, h * z.sum_rows)
            grad_t += item_grad(u16, error)
            g_ref[...] = user_grad(error, vt16)
        write_panel(z, m_ref, updated(vt, step, grad_t), step)

    half = jax.ShapeDtypeStruct((z.half, z.rank), f32)
    return pl.pallas_call(
        body,
        in_specs=[smem] + [hbm] * 7,
        out_specs=[vmem] * 4,
        out_shape=[jax.ShapeDtypeStruct((z.panel_rows, z.tile), f32), half, half, half],
        scratch_shapes=[
            pltpu.VMEM((z.slots, z.tile, z.tile), bf16),
            pltpu.VMEM((2 * z.sum_rows, z.tile), f32),
            pltpu.VMEM((z.half, z.rank), f32),
            pltpu.VMEM((z.items, z.rank), f32),
            pltpu.VMEM(item_count.shape, jnp.int32),
            pltpu.SMEM(tiles[0].shape, jnp.int32),
            pltpu.SMEM(tiles[1].shape, jnp.int32),
            pltpu.SMEM(tiles[2].shape, jnp.int32),
            pltpu.SemaphoreType.DMA((z.slots // group,)),
            pltpu.SemaphoreType.DMA((4,)),
            pltpu.SemaphoreType.DMA((3,)),
        ],
        compiler_params=pltpu.CompilerParams(vmem_limit_bytes=28 * 2**20),
        cost_estimate=visit_cost(z, 6),
        name="first_visit",
    )(side, *tiles, ratings, user_factors, item_factors, item_count)


def user_visit(z, own, panel, partner_panel, s_own, s_partner):
    def body(own_ref, m_ref, x_ref, so_ref, sx_ref, g_ref, share_ref):
        own16 = own_ref[...].astype(bf16)
        xt16 = read_panel(z, x_ref).astype(bf16)
        vt16 = read_panel(z, m_ref).astype(bf16)
        error = errors(z, own16, vt16, so_ref)
        grad = user_grad(error, vt16)
        g_ref[...] = grad + user_grad(errors(z, own16, xt16, sx_ref), xt16)
        share_ref[...] = item_grad(own16, error)

    return pl.pallas_call(
        body,
        in_specs=[vmem] * 5,
        out_specs=[vmem] * 2,
        out_shape=[
            jax.ShapeDtypeStruct((z.half, z.rank), f32),
            jax.ShapeDtypeStruct((z.rank, z.items), f32),
        ],
        compiler_params=pltpu.CompilerParams(vmem_limit_bytes=24 * 2**20),
        cost_estimate=visit_cost(z, 5),
        name="user_visit",
    )(own, panel, partner_panel, s_own, s_partner)


def panel_visit(z, other, panel, share, s_oth, last):
    def body(oth_ref, m_ref, share_ref, st_ref, mout_ref):
        vt = read_panel(z, m_ref)
        step = read_steps(z, m_ref)
        oth16 = oth_ref[...].astype(bf16)
        grad_t = share_ref[...] + item_grad(oth16, errors(z, oth16, vt.astype(bf16), st_ref))
        vnew = updated(vt, step, grad_t)
        if last:
            for c in range(z.col_tiles):
                cols = slice(c * z.tile, (c + 1) * z.tile)
                mout_ref[c * z.tile : (c + 1) * z.tile, :] = vnew[:, cols].T
        else:
            write_panel(z, mout_ref, vnew, step)

    rows = z.items if last else z.panel_rows
    return pl.pallas_call(
        body,
        in_specs=[vmem] * 4,
        out_specs=vmem,
        out_shape=jax.ShapeDtypeStruct((rows, z.tile), f32),
        compiler_params=pltpu.CompilerParams(vmem_limit_bytes=24 * 2**20),
        cost_estimate=visit_cost(z, 2),
        name="panel_visit",
    )(other, panel, share, s_oth)


def outputs(z, side, own, other, panel):
    def body(side_ref, own_ref, oth_ref, v_ref, u_hbm, v_hbm, sems):
        side = side_ref[0]
        own_at = pl.multiple_of(side * z.half, z.half)
        oth_at = pl.multiple_of((1 - side) * z.half, z.half)
        copies = [
            pltpu.make_async_copy(own_ref, u_hbm.at[pl.ds(own_at, z.half)], sems.at[0]),
            pltpu.make_async_copy(oth_ref, u_hbm.at[pl.ds(oth_at, z.half)], sems.at[1]),
            pltpu.make_async_copy(v_ref, v_hbm, sems.at[2]),
        ]
        for copy in copies:
            copy.start()
        for copy in copies:
            copy.wait()

    return pl.pallas_call(
        body,
        in_specs=[smem, vmem, vmem, vmem],
        out_specs=[hbm, hbm],
        out_shape=[
            jax.ShapeDtypeStruct((z.users, z.rank), f32),
            jax.ShapeDtypeStruct((z.items, z.rank), f32),
        ],
        scratch_shapes=[pltpu.SemaphoreType.DMA((3,))],
        compiler_params=pltpu.CompilerParams(vmem_limit_bytes=8 * 2**20),
        name="outputs",
    )(side, own, other, panel)


def per_device(
    ratings, user_tile, item_tile, tile_count, user_count, item_count, user_factors, item_factors
):
    z = Sizes(ratings, user_factors, item_factors)
    core = lax.axis_index("split") % 2
    side = core.astype(jnp.int32).reshape(1)
    tiles = (user_tile, item_tile, tile_count.reshape(-1))
    ratings, user_factors, item_factors = (
        pltpu.with_memory_space_constraint(x, pltpu.HBM)
        for x in (ratings, user_factors, item_factors)
    )

    item_count = item_count.reshape(-1, z.tile)
    fixed = [pltpu.with_memory_space_constraint(x, pltpu.HBM) for x in (*tiles, item_count)]
    panel, grad, grad_other, own = first_visit(
        z, side, fixed[:3], ratings, user_factors, item_factors, fixed[3]
    )
    for visit_no in range(z.visits):
        last = visit_no == z.visits - 1
        if visit_no == 0:
            grad = grad + swapped(grad_other, "split", 1)
        else:
            partner_panel = swapped(panel, "split", 1)
            own = own + own_step * (grad + crossed - decay_rate * own)
            other = swapped(own, "split", 1)
            grad, share = user_visit(z, own, panel, partner_panel, s_own, s_partner)
        crossed = swapped(grad, "split", 2)
        if visit_no > 0:
            panel = panel_visit(z, other, panel, share, s_oth, last)
        panel = from_ahead(panel, "blk", 1 - z.visits if last else 1)
        if not last:
            if visit_no == 0:
                s_own, s_oth, own_step = pair_sums(
                    z, 1, side, tiles, ratings, grad, user_count, lax.axis_size("split")
                )
            else:
                s_own, s_oth = pair_sums(z, visit_no + 1, side, tiles, ratings, grad)
            s_partner = swapped(s_oth, "split", 1)
    own = own + own_step * (grad + crossed - decay_rate * own)
    other = swapped(own, "split", 1)
    return outputs(z, side, own, other, panel)


def solution(mesh):
    return jax.shard_map(
        per_device,
        mesh=mesh,
        in_specs=(
            P("blk", None, "split", None, None, None),
            P("blk", None, "split", None),
            P("blk", None, "split", None),
            P("blk", None, "split"),
            P("blk"),
            P(("blk", "split")),
            P("blk", None),
            P(("blk", "split"), None),
        ),
        out_specs=(P("blk", None), P(("blk", "split"), None)),
        check_vma=False,
    )
```

```python
import jax
import jax.numpy as jnp
from jax import lax
from jax.experimental import pallas as pl
from jax.experimental.pallas import tpu as pltpu
from jax.sharding import PartitionSpec as P


step_gain = 12.0
decay_rate = 0.05
group = 8
chunk = 2
f32, bf16 = jnp.float32, jnp.bfloat16
hbm = pl.BlockSpec(memory_space=pltpu.HBM)
smem = pl.BlockSpec(memory_space=pltpu.SMEM)
vmem = pl.BlockSpec(memory_space=pltpu.VMEM)


def from_ahead(x, axis, by):
    peers = lax.axis_size(axis)
    return lax.ppermute(x, axis, [(i, (i - by) % peers) for i in range(peers)])


def swapped(x, axis, bit):
    peers = lax.axis_size(axis)
    return lax.ppermute(x, axis, [(i, i ^ bit) for i in range(peers)])


class Sizes:
    def __init__(self, ratings, user_factors, item_factors):
        self.visits, self.slots, self.tile = ratings.shape[1], ratings.shape[3], ratings.shape[-1]
        self.users, self.rank = user_factors.shape
        self.items = item_factors.shape[0]
        self.half = self.users // 2
        self.row_tiles, self.col_tiles = self.half // self.tile, self.items // self.tile
        self.half_pairs = self.row_tiles * self.col_tiles
        self.sum_rows = self.half_pairs * self.tile + self.half_pairs
        self.panel_rows = self.items + -(-self.col_tiles // 8) * 8


def group_copy(visit_no, r_hbm, buf, sems, g):
    slots = pl.ds(g * group, group)
    return pltpu.make_async_copy(r_hbm.at[0, visit_no, 0, slots], buf.at[slots], sems.at[g])


def start_live(z, visit_no, live, r_hbm, buf, sems):
    for g in range(z.slots // group):
        @pl.when(g * group < live)
        def _():
            group_copy(visit_no, r_hbm, buf, sems, g).start()


def add_live(z, visit_no, side, live, ut, it, r_hbm, buf, sems, sum_ref):
    sum_ref[...] = jnp.zeros_like(sum_ref)
    count_row = z.half_pairs * z.tile

    def add_slot(t):
        user = ut[0, visit_no, 0, t] + side * z.row_tiles
        user = jnp.where(user >= 2 * z.row_tiles, user - 2 * z.row_tiles, user)
        half = jnp.where(user >= z.row_tiles, 1, 0)
        pair = (user - half * z.row_tiles) * z.col_tiles + it[0, visit_no, 0, t]
        row = pl.multiple_of(half * z.sum_rows + pair * z.tile, 8)
        sum_ref[pl.ds(row, z.tile), :] += buf[t].astype(f32)
        sum_ref[pl.ds(half * z.sum_rows + count_row + pair, 1), :] += 1.0

    def add_group(g, carry):
        group_copy(visit_no, r_hbm, buf, sems, g).wait()
        for i in range(group):
            add_slot(g * group + i)
        return carry

    def add_one(t, carry):
        add_slot(t)
        return carry

    full = live // group
    lax.fori_loop(0, full, add_group, 0)

    @pl.when(full * group < live)
    def _():
        group_copy(visit_no, r_hbm, buf, sems, full).wait()
        lax.fori_loop(full * group, live, add_one, 0)


def pair_sums(z, visit_no, side, tiles, ratings, after, user_count=None, split_count=None):
    with_steps = user_count is not None

    def body(side_ref, ut, it, cnt, r_hbm, _, *refs):
        live = cnt[visit_no]
        if with_steps:
            count_ref, own_ref, oth_ref, step_ref, buf, sum_ref, sems = refs
        else:
            own_ref, oth_ref, buf, sum_ref, sems = refs
        start_live(z, visit_no, live, r_hbm, buf, sems)
        if with_steps:
            user_norm = z.slots * z.tile * z.tile * split_count / z.users
            for a in range(z.row_tiles):
                count = count_ref[pl.ds(side_ref[0] * z.row_tiles + a, 1), :].astype(f32)
                step = step_gain / (user_norm * jnp.sqrt(count))
                rows = jnp.broadcast_to(step, (z.tile, z.tile)).T
                step_ref[a * z.tile : (a + 1) * z.tile, :] = rows
        add_live(z, visit_no, side_ref[0], live, ut, it, r_hbm, buf, sems, sum_ref)
        own_ref[...] = sum_ref[: z.sum_rows, :]
        oth_ref[...] = sum_ref[z.sum_rows :, :]

    out = jax.ShapeDtypeStruct((z.sum_rows, z.tile), f32)
    return pl.pallas_call(
        body,
        in_specs=[smem] * 4 + [hbm, pl.BlockSpec(memory_space=pl.ANY)] + [vmem] * with_steps,
        out_specs=[vmem] * (2 + with_steps),
        out_shape=[out, out] + [jax.ShapeDtypeStruct((z.half, z.rank), f32)] * with_steps,
        scratch_shapes=[
            pltpu.VMEM((z.slots, z.tile, z.tile), bf16),
            pltpu.VMEM((2 * z.sum_rows, z.tile), f32),
            pltpu.SemaphoreType.DMA((z.slots // group,)),
        ],
        compiler_params=pltpu.CompilerParams(vmem_limit_bytes=16 * 2**20),
        cost_estimate=pl.CostEstimate(
            flops=z.slots * z.tile * z.tile * 4,
            transcendentals=0,
            bytes_accessed=z.slots * z.tile * z.tile * 2,
        ),
        name="pair_sums",
    )(side, *tiles, ratings, after, *([user_count.reshape(-1, z.tile)] if with_steps else []))


def errors(z, u16, vt16, s_ref, base=0, tiles=None):
    predicted = jnp.dot(u16, vt16, preferred_element_type=f32)
    return errors_of(z, predicted, s_ref, base, tiles)


def errors_of(z, predicted, s_ref, base, tiles):
    count_row = base + z.half_pairs * z.tile
    first, number = tiles or (0, z.row_tiles)
    rows = []
    for a in range(number):
        cols = []
        for c in range(z.col_tiles):
            pair = (first + a) * z.col_tiles + c
            part = predicted[a * z.tile : (a + 1) * z.tile, c * z.tile : (c + 1) * z.tile]
            sums = s_ref[base + pair * z.tile : base + (pair + 1) * z.tile, :]
            count = s_ref[count_row + pair : count_row + pair + 1, :]
            cols.append((sums - count * part).astype(bf16))
        rows.append(jnp.concatenate(cols, axis=1))
    return jnp.concatenate(rows, axis=0)


def user_grad(error, vt16):
    return lax.dot_general(error, vt16, (((1,), (1,)), ((), ())), preferred_element_type=f32)


def item_grad(u16, error):
    return lax.dot_general(u16, error, (((0,), (0,)), ((), ())), preferred_element_type=f32)


def read_panel(z, m_ref):
    blocks = [m_ref[c * z.tile : (c + 1) * z.tile, :] for c in range(z.col_tiles)]
    return jnp.concatenate(blocks, axis=1)


def read_steps(z, m_ref):
    return jnp.concatenate([m_ref[z.items + c : z.items + c + 1, :] for c in range(z.col_tiles)], axis=1)


def write_panel(z, m_ref, vt, step):
    m_ref[z.items :, :] = jnp.zeros((z.panel_rows - z.items, z.tile), f32)
    for c in range(z.col_tiles):
        cols = slice(c * z.tile, (c + 1) * z.tile)
        m_ref[c * z.tile : (c + 1) * z.tile, :] = vt[:, cols]
        m_ref[z.items + c : z.items + c + 1, :] = step[:, cols]


def updated(vt, step, grad_t):
    return vt + step * (grad_t - decay_rate * vt)


def visit_cost(z, quarters):
    flops = 2 * z.half * z.items * z.rank * quarters
    return pl.CostEstimate(flops=flops, transcendentals=0, bytes_accessed=4 * 2**20)


def first_visit(z, side, tiles, ratings, user_factors, item_factors, item_count):
    def body(
        side_ref, ut_hbm, it_hbm, cnt_hbm, r_hbm, u_hbm, v_hbm, ic_hbm,
        m_ref, gown_ref, goth_ref, own_ref,
        buf, sum_ref, pred_ref, vt_ref, oth_ref, v_ref, ic_ref, ut, it, cnt, sems, fsems, isems,
    ):
        side = side_ref[0]
        indices = [
            pltpu.make_async_copy(src, dst, isems.at[i])
            for i, (src, dst) in enumerate(((cnt_hbm, cnt), (ut_hbm, ut), (it_hbm, it)))
        ]
        own_at = pl.multiple_of(side * z.half, z.half)
        oth_at = pl.multiple_of((1 - side) * z.half, z.half)
        factors = [
            pltpu.make_async_copy(v_hbm, v_ref, fsems.at[0]),
            pltpu.make_async_copy(ic_hbm, ic_ref, fsems.at[1]),
            pltpu.make_async_copy(u_hbm.at[pl.ds(own_at, z.half)], own_ref, fsems.at[2]),
            pltpu.make_async_copy(u_hbm.at[pl.ds(oth_at, z.half)], oth_ref, fsems.at[3]),
        ]
        groups = z.slots // group
        for copy in indices + factors:
            copy.start()
        for g in range(groups):
            group_copy(0, r_hbm, buf, sems, g).start()
        for copy in factors[:2]:
            copy.wait()
        item_norm = z.slots * z.tile * z.tile / z.items
        step = step_gain / (item_norm * jnp.sqrt(ic_ref[...].astype(f32)))
        step = jnp.concatenate([step[c : c + 1, :] for c in range(z.col_tiles)], axis=1)
        for c in range(z.col_tiles):
            cols = slice(c * z.tile, (c + 1) * z.tile)
            vt_ref[:, cols] = v_ref[cols, :].T
        vt16 = vt_ref[...].astype(bf16)
        for copy in factors[2:]:
            copy.wait()
        for h, u_ref in enumerate((own_ref, oth_ref)):
            u16 = u_ref[...].astype(bf16)
            pred_ref[h * z.half : (h + 1) * z.half, :] = jnp.dot(u16, vt16, preferred_element_type=f32)
        for copy in indices:
            copy.wait()
        live = cnt[0]
        add_live(z, 0, side, live, ut, it, r_hbm, buf, sems, sum_ref)

        def drop(g, carry):
            group_copy(0, r_hbm, buf, sems, g).wait()
            return carry

        lax.fori_loop((live + group - 1) // group, groups, drop, 0)
        vt = vt_ref[...]
        vt16 = vt.astype(bf16)
        grad_t = jnp.zeros((z.rank, z.items), f32)
        for h, (u_ref, g_ref) in enumerate(((own_ref, gown_ref), (oth_ref, goth_ref))):
            for at in range(0, z.row_tiles, chunk):
                rows = slice(at * z.tile, (at + chunk) * z.tile)
                u16 = u_ref[rows, :].astype(bf16)
                base = h * z.half + at * z.tile
                predicted = pred_ref[base : base + chunk * z.tile, :]
                error = errors_of(z, predicted, sum_ref, h * z.sum_rows, (at, chunk))
                grad_t += item_grad(u16, error)
                g_ref[rows, :] = user_grad(error, vt16)
        write_panel(z, m_ref, updated(vt, step, grad_t), step)

    half = jax.ShapeDtypeStruct((z.half, z.rank), f32)
    return pl.pallas_call(
        body,
        in_specs=[smem] + [hbm] * 7,
        out_specs=[vmem] * 4,
        out_shape=[jax.ShapeDtypeStruct((z.panel_rows, z.tile), f32), half, half, half],
        scratch_shapes=[
            pltpu.VMEM((z.slots, z.tile, z.tile), bf16),
            pltpu.VMEM((2 * z.sum_rows, z.tile), f32),
            pltpu.VMEM((z.users, z.items), f32),
            pltpu.VMEM((z.rank, z.items), f32),
            pltpu.VMEM((z.half, z.rank), f32),
            pltpu.VMEM((z.items, z.rank), f32),
            pltpu.VMEM(item_count.shape, jnp.int32),
            pltpu.SMEM(tiles[0].shape, jnp.int32),
            pltpu.SMEM(tiles[1].shape, jnp.int32),
            pltpu.SMEM(tiles[2].shape, jnp.int32),
            pltpu.SemaphoreType.DMA((z.slots // group,)),
            pltpu.SemaphoreType.DMA((4,)),
            pltpu.SemaphoreType.DMA((3,)),
        ],
        compiler_params=pltpu.CompilerParams(vmem_limit_bytes=28 * 2**20),
        cost_estimate=visit_cost(z, 6),
        name="first_visit",
    )(side, *tiles, ratings, user_factors, item_factors, item_count)


def user_visit(z, own, panel, partner_panel, s_own, s_partner):
    def body(own_ref, m_ref, x_ref, so_ref, sx_ref, g_ref, share_ref):
        xt16 = read_panel(z, x_ref).astype(bf16)
        vt16 = read_panel(z, m_ref).astype(bf16)
        share = jnp.zeros((z.rank, z.items), f32)
        for first in range(0, z.row_tiles, chunk):
            rows = slice(first * z.tile, (first + chunk) * z.tile)
            own16 = own_ref[rows, :].astype(bf16)
            error = errors(z, own16, vt16, so_ref, tiles=(first, chunk))
            far = errors(z, own16, xt16, sx_ref, tiles=(first, chunk))
            g_ref[rows, :] = user_grad(error, vt16) + user_grad(far, xt16)
            share += item_grad(own16, error)
        share_ref[...] = share

    return pl.pallas_call(
        body,
        in_specs=[vmem] * 5,
        out_specs=[vmem] * 2,
        out_shape=[
            jax.ShapeDtypeStruct((z.half, z.rank), f32),
            jax.ShapeDtypeStruct((z.rank, z.items), f32),
        ],
        compiler_params=pltpu.CompilerParams(vmem_limit_bytes=24 * 2**20),
        cost_estimate=visit_cost(z, 5),
        name="user_visit",
    )(own, panel, partner_panel, s_own, s_partner)


def panel_visit(z, other, panel, share, s_oth, last):
    def body(oth_ref, m_ref, share_ref, st_ref, mout_ref):
        vt = read_panel(z, m_ref)
        step = read_steps(z, m_ref)
        oth16 = oth_ref[...].astype(bf16)
        grad_t = share_ref[...] + item_grad(oth16, errors(z, oth16, vt.astype(bf16), st_ref))
        vnew = updated(vt, step, grad_t)
        if last:
            for c in range(z.col_tiles):
                cols = slice(c * z.tile, (c + 1) * z.tile)
                mout_ref[c * z.tile : (c + 1) * z.tile, :] = vnew[:, cols].T
        else:
            write_panel(z, mout_ref, vnew, step)

    rows = z.items if last else z.panel_rows
    return pl.pallas_call(
        body,
        in_specs=[vmem] * 4,
        out_specs=vmem,
        out_shape=jax.ShapeDtypeStruct((rows, z.tile), f32),
        compiler_params=pltpu.CompilerParams(vmem_limit_bytes=24 * 2**20),
        cost_estimate=visit_cost(z, 2),
        name="panel_visit",
    )(other, panel, share, s_oth)


def outputs(z, side, own, other, panel):
    def body(side_ref, own_ref, oth_ref, v_ref, u_hbm, v_hbm, sems):
        side = side_ref[0]
        own_at = pl.multiple_of(side * z.half, z.half)
        oth_at = pl.multiple_of((1 - side) * z.half, z.half)
        copies = [
            pltpu.make_async_copy(own_ref, u_hbm.at[pl.ds(own_at, z.half)], sems.at[0]),
            pltpu.make_async_copy(oth_ref, u_hbm.at[pl.ds(oth_at, z.half)], sems.at[1]),
            pltpu.make_async_copy(v_ref, v_hbm, sems.at[2]),
        ]
        for copy in copies:
            copy.start()
        for copy in copies:
            copy.wait()

    return pl.pallas_call(
        body,
        in_specs=[smem, vmem, vmem, vmem],
        out_specs=[hbm, hbm],
        out_shape=[
            jax.ShapeDtypeStruct((z.users, z.rank), f32),
            jax.ShapeDtypeStruct((z.items, z.rank), f32),
        ],
        scratch_shapes=[pltpu.SemaphoreType.DMA((3,))],
        compiler_params=pltpu.CompilerParams(vmem_limit_bytes=8 * 2**20),
        name="outputs",
    )(side, own, other, panel)


def per_device(
    ratings, user_tile, item_tile, tile_count, user_count, item_count, user_factors, item_factors
):
    z = Sizes(ratings, user_factors, item_factors)
    core = lax.axis_index("split") % 2
    side = core.astype(jnp.int32).reshape(1)
    tiles = (user_tile, item_tile, tile_count.reshape(-1))
    ratings, user_factors, item_factors = (
        pltpu.with_memory_space_constraint(x, pltpu.HBM)
        for x in (ratings, user_factors, item_factors)
    )

    item_count = item_count.reshape(-1, z.tile)
    fixed = [pltpu.with_memory_space_constraint(x, pltpu.HBM) for x in (*tiles, item_count)]
    panel, grad, grad_other, own = first_visit(
        z, side, fixed[:3], ratings, user_factors, item_factors, fixed[3]
    )
    for visit_no in range(z.visits):
        last = visit_no == z.visits - 1
        if visit_no == 0:
            grad = grad + swapped(grad_other, "split", 1)
        else:
            partner_panel = swapped(panel, "split", 1)
            own = own + own_step * (grad + crossed - decay_rate * own)
            other = swapped(own, "split", 1)
            grad, share = user_visit(z, own, panel, partner_panel, s_own, s_partner)
        crossed = swapped(grad, "split", 2)
        if visit_no > 0:
            panel = panel_visit(z, other, panel, share, s_oth, last)
        panel = from_ahead(panel, "blk", 1 - z.visits if last else 1)
        if not last:
            if visit_no == 0:
                s_own, s_oth, own_step = pair_sums(
                    z, 1, side, tiles, ratings, grad, user_count, lax.axis_size("split")
                )
            else:
                s_own, s_oth = pair_sums(z, visit_no + 1, side, tiles, ratings, grad)
            s_partner = swapped(s_oth, "split", 1)
    own = own + own_step * (grad + crossed - decay_rate * own)
    other = swapped(own, "split", 1)
    return outputs(z, side, own, other, panel)


def solution(mesh):
    return jax.shard_map(
        per_device,
        mesh=mesh,
        in_specs=(
            P("blk", None, "split", None, None, None),
            P("blk", None, "split", None),
            P("blk", None, "split", None),
            P("blk", None, "split"),
            P("blk"),
            P(("blk", "split")),
            P("blk", None),
            P(("blk", "split"), None),
        ),
        out_specs=(P("blk", None), P(("blk", "split"), None)),
        check_vma=False,
    )
```

```python
import jax
import jax.numpy as jnp
from jax import lax
from jax.experimental import pallas as pl
from jax.experimental.pallas import tpu as pltpu
from jax.sharding import PartitionSpec as P


step_gain = 12.0
decay_rate = 0.05
group = 8
chunk = 2
f32, bf16 = jnp.float32, jnp.bfloat16
hbm = pl.BlockSpec(memory_space=pltpu.HBM)
smem = pl.BlockSpec(memory_space=pltpu.SMEM)
vmem = pl.BlockSpec(memory_space=pltpu.VMEM)


def from_ahead(x, axis, by):
    peers = lax.axis_size(axis)
    return lax.ppermute(x, axis, [(i, (i - by) % peers) for i in range(peers)])


def swapped(x, axis, bit):
    peers = lax.axis_size(axis)
    return lax.ppermute(x, axis, [(i, i ^ bit) for i in range(peers)])


class Sizes:
    def __init__(self, ratings, user_factors, item_factors):
        self.visits, self.slots, self.tile = ratings.shape[1], ratings.shape[3], ratings.shape[-1]
        self.users, self.rank = user_factors.shape
        self.items = item_factors.shape[0]
        self.half = self.users // 2
        self.row_tiles, self.col_tiles = self.half // self.tile, self.items // self.tile
        self.half_pairs = self.row_tiles * self.col_tiles
        self.sum_rows = self.half_pairs * self.tile + self.half_pairs
        self.panel_rows = self.items + -(-self.col_tiles // 8) * 8


def group_copy(visit_no, r_hbm, buf, sems, g):
    slots = pl.ds(g * group, group)
    return pltpu.make_async_copy(r_hbm.at[0, visit_no, 0, slots], buf.at[slots], sems.at[g])


def start_live(z, visit_no, live, r_hbm, buf, sems):
    for g in range(z.slots // group):
        @pl.when(g * group < live)
        def _():
            group_copy(visit_no, r_hbm, buf, sems, g).start()


def add_live(z, visit_no, side, live, ut, it, r_hbm, buf, sems, *sum_refs):
    count_row = z.half_pairs * z.tile

    def add_slot(t, sum_ref=sum_refs[0]):
        user = ut[0, visit_no, 0, t] + side * z.row_tiles
        user = jnp.where(user >= 2 * z.row_tiles, user - 2 * z.row_tiles, user)
        half = jnp.where(user >= z.row_tiles, 1, 0)
        pair = (user - half * z.row_tiles) * z.col_tiles + it[0, visit_no, 0, t]
        row = pl.multiple_of(half * z.sum_rows + pair * z.tile, 8)
        sum_ref[pl.ds(row, z.tile), :] += buf[t].astype(f32)
        sum_ref[pl.ds(half * z.sum_rows + count_row + pair, 1), :] += 1.0

    def add_group(g, carry):
        group_copy(visit_no, r_hbm, buf, sems, g).wait()
        for i in range(group):
            add_slot(g * group + i, sum_refs[i % len(sum_refs)])
        return carry

    def add_one(t, carry):
        add_slot(t)
        return carry

    full = live // group
    lax.fori_loop(0, full, add_group, 0)

    @pl.when(full * group < live)
    def _():
        group_copy(visit_no, r_hbm, buf, sems, full).wait()
        lax.fori_loop(full * group, live, add_one, 0)


def pair_sums(z, visit_no, side, tiles, ratings, after, user_count=None, split_count=None):
    with_steps = user_count is not None

    def body(side_ref, ut, it, cnt, r_hbm, _, *refs):
        live = cnt[visit_no]
        if with_steps:
            count_ref, own_ref, oth_ref, step_ref, buf, sum_ref, sems = refs
        else:
            own_ref, oth_ref, buf, sum_ref, sems = refs
        start_live(z, visit_no, live, r_hbm, buf, sems)
        sum_ref[...] = jnp.zeros_like(sum_ref)
        if with_steps:
            user_norm = z.slots * z.tile * z.tile * split_count / z.users
            for a in range(z.row_tiles):
                count = count_ref[pl.ds(side_ref[0] * z.row_tiles + a, 1), :].astype(f32)
                step = step_gain / (user_norm * jnp.sqrt(count))
                rows = jnp.broadcast_to(step, (z.tile, z.tile)).T
                step_ref[a * z.tile : (a + 1) * z.tile, :] = rows
        add_live(z, visit_no, side_ref[0], live, ut, it, r_hbm, buf, sems, sum_ref)
        own_ref[...] = sum_ref[: z.sum_rows, :]
        oth_ref[...] = sum_ref[z.sum_rows :, :]

    out = jax.ShapeDtypeStruct((z.sum_rows, z.tile), f32)
    return pl.pallas_call(
        body,
        in_specs=[smem] * 4 + [hbm, pl.BlockSpec(memory_space=pl.ANY)] + [vmem] * with_steps,
        out_specs=[vmem] * (2 + with_steps),
        out_shape=[out, out] + [jax.ShapeDtypeStruct((z.half, z.rank), f32)] * with_steps,
        scratch_shapes=[
            pltpu.VMEM((z.slots, z.tile, z.tile), bf16),
            pltpu.VMEM((2 * z.sum_rows, z.tile), f32),
            pltpu.SemaphoreType.DMA((z.slots // group,)),
        ],
        compiler_params=pltpu.CompilerParams(vmem_limit_bytes=16 * 2**20),
        cost_estimate=pl.CostEstimate(
            flops=z.slots * z.tile * z.tile * 4,
            transcendentals=0,
            bytes_accessed=z.slots * z.tile * z.tile * 2,
        ),
        name="pair_sums",
    )(side, *tiles, ratings, after, *([user_count.reshape(-1, z.tile)] if with_steps else []))


def errors(z, u16, vt16, s_ref, base=0, tiles=None):
    predicted = jnp.dot(u16, vt16, preferred_element_type=f32)
    return errors_of(z, predicted, s_ref, base, tiles)


def errors_of(z, predicted, s_ref, base, tiles, more_ref=None):
    count_row = base + z.half_pairs * z.tile
    first, number = tiles or (0, z.row_tiles)
    rows = []
    for a in range(number):
        cols = []
        for c in range(z.col_tiles):
            pair = (first + a) * z.col_tiles + c
            part = predicted[a * z.tile : (a + 1) * z.tile, c * z.tile : (c + 1) * z.tile]
            rows_at = slice(base + pair * z.tile, base + (pair + 1) * z.tile)
            count_at = slice(count_row + pair, count_row + pair + 1)
            sums, count = s_ref[rows_at, :], s_ref[count_at, :]
            if more_ref is not None:
                sums, count = sums + more_ref[rows_at, :], count + more_ref[count_at, :]
            cols.append((sums - count * part).astype(bf16))
        rows.append(jnp.concatenate(cols, axis=1))
    return jnp.concatenate(rows, axis=0)


def user_grad(error, vt16):
    return lax.dot_general(error, vt16, (((1,), (1,)), ((), ())), preferred_element_type=f32)


def item_grad(u16, error):
    return lax.dot_general(u16, error, (((0,), (0,)), ((), ())), preferred_element_type=f32)


def read_panel(z, m_ref):
    blocks = [m_ref[c * z.tile : (c + 1) * z.tile, :] for c in range(z.col_tiles)]
    return jnp.concatenate(blocks, axis=1)


def read_steps(z, m_ref):
    return jnp.concatenate([m_ref[z.items + c : z.items + c + 1, :] for c in range(z.col_tiles)], axis=1)


def write_panel(z, m_ref, vt, step):
    m_ref[z.items :, :] = jnp.zeros((z.panel_rows - z.items, z.tile), f32)
    for c in range(z.col_tiles):
        cols = slice(c * z.tile, (c + 1) * z.tile)
        m_ref[c * z.tile : (c + 1) * z.tile, :] = vt[:, cols]
        m_ref[z.items + c : z.items + c + 1, :] = step[:, cols]


def updated(vt, step, grad_t):
    return vt + step * (grad_t - decay_rate * vt)


def visit_cost(z, quarters):
    flops = 2 * z.half * z.items * z.rank * quarters
    return pl.CostEstimate(flops=flops, transcendentals=0, bytes_accessed=4 * 2**20)


def first_visit(z, side, tiles, ratings, user_factors, item_factors, item_count):
    def body(
        side_ref, ut_hbm, it_hbm, cnt_hbm, r_hbm, u_hbm, v_hbm, ic_hbm,
        m_ref, gown_ref, goth_ref, own_ref,
        buf, sum_ref, more_ref, pred_ref, vt_ref, oth_ref, v_ref, ic_ref, ut, it, cnt, sems, fsems, isems,
    ):
        side = side_ref[0]
        indices = [
            pltpu.make_async_copy(src, dst, isems.at[i])
            for i, (src, dst) in enumerate(((cnt_hbm, cnt), (ut_hbm, ut), (it_hbm, it)))
        ]
        own_at = pl.multiple_of(side * z.half, z.half)
        oth_at = pl.multiple_of((1 - side) * z.half, z.half)
        factors = [
            pltpu.make_async_copy(v_hbm, v_ref, fsems.at[0]),
            pltpu.make_async_copy(ic_hbm, ic_ref, fsems.at[1]),
            pltpu.make_async_copy(u_hbm.at[pl.ds(own_at, z.half)], own_ref, fsems.at[2]),
            pltpu.make_async_copy(u_hbm.at[pl.ds(oth_at, z.half)], oth_ref, fsems.at[3]),
        ]
        groups = z.slots // group
        for copy in indices + factors:
            copy.start()
        for g in range(groups):
            group_copy(0, r_hbm, buf, sems, g).start()
        sum_ref[...] = jnp.zeros_like(sum_ref)
        more_ref[...] = jnp.zeros_like(more_ref)
        for copy in factors[:2]:
            copy.wait()
        item_norm = z.slots * z.tile * z.tile / z.items
        step = step_gain / (item_norm * jnp.sqrt(ic_ref[...].astype(f32)))
        step = jnp.concatenate([step[c : c + 1, :] for c in range(z.col_tiles)], axis=1)
        for c in range(z.col_tiles):
            cols = slice(c * z.tile, (c + 1) * z.tile)
            vt_ref[:, cols] = v_ref[cols, :].T
        vt16 = vt_ref[...].astype(bf16)
        for copy in factors[2:]:
            copy.wait()
        for h, u_ref in enumerate((own_ref, oth_ref)):
            u16 = u_ref[...].astype(bf16)
            pred_ref[h * z.half : (h + 1) * z.half, :] = jnp.dot(u16, vt16, preferred_element_type=f32)
        for copy in indices:
            copy.wait()
        live = cnt[0]
        add_live(z, 0, side, live, ut, it, r_hbm, buf, sems, sum_ref, more_ref)

        def drop(g, carry):
            group_copy(0, r_hbm, buf, sems, g).wait()
            return carry

        lax.fori_loop((live + group - 1) // group, groups, drop, 0)
        vt = vt_ref[...]
        vt16 = vt.astype(bf16)
        grad_t = jnp.zeros((z.rank, z.items), f32)
        for h, (u_ref, g_ref) in enumerate(((own_ref, gown_ref), (oth_ref, goth_ref))):
            for at in range(0, z.row_tiles, chunk):
                rows = slice(at * z.tile, (at + chunk) * z.tile)
                u16 = u_ref[rows, :].astype(bf16)
                base = h * z.half + at * z.tile
                predicted = pred_ref[base : base + chunk * z.tile, :]
                error = errors_of(z, predicted, sum_ref, h * z.sum_rows, (at, chunk), more_ref)
                grad_t += item_grad(u16, error)
                g_ref[rows, :] = user_grad(error, vt16)
        write_panel(z, m_ref, updated(vt, step, grad_t), step)

    half = jax.ShapeDtypeStruct((z.half, z.rank), f32)
    return pl.pallas_call(
        body,
        in_specs=[smem] + [hbm] * 7,
        out_specs=[vmem] * 4,
        out_shape=[jax.ShapeDtypeStruct((z.panel_rows, z.tile), f32), half, half, half],
        scratch_shapes=[
            pltpu.VMEM((z.slots, z.tile, z.tile), bf16),
            pltpu.VMEM((2 * z.sum_rows, z.tile), f32),
            pltpu.VMEM((2 * z.sum_rows, z.tile), f32),
            pltpu.VMEM((z.users, z.items), f32),
            pltpu.VMEM((z.rank, z.items), f32),
            pltpu.VMEM((z.half, z.rank), f32),
            pltpu.VMEM((z.items, z.rank), f32),
            pltpu.VMEM(item_count.shape, jnp.int32),
            pltpu.SMEM(tiles[0].shape, jnp.int32),
            pltpu.SMEM(tiles[1].shape, jnp.int32),
            pltpu.SMEM(tiles[2].shape, jnp.int32),
            pltpu.SemaphoreType.DMA((z.slots // group,)),
            pltpu.SemaphoreType.DMA((4,)),
            pltpu.SemaphoreType.DMA((3,)),
        ],
        compiler_params=pltpu.CompilerParams(vmem_limit_bytes=28 * 2**20),
        cost_estimate=visit_cost(z, 6),
        name="first_visit",
    )(side, *tiles, ratings, user_factors, item_factors, item_count)


def user_visit(z, own, panel, partner_panel, s_own, s_partner):
    def body(own_ref, m_ref, x_ref, so_ref, sx_ref, g_ref, share_ref):
        xt16 = read_panel(z, x_ref).astype(bf16)
        vt16 = read_panel(z, m_ref).astype(bf16)
        share = jnp.zeros((z.rank, z.items), f32)
        for first in range(0, z.row_tiles, chunk):
            rows = slice(first * z.tile, (first + chunk) * z.tile)
            own16 = own_ref[rows, :].astype(bf16)
            error = errors(z, own16, vt16, so_ref, tiles=(first, chunk))
            far = errors(z, own16, xt16, sx_ref, tiles=(first, chunk))
            g_ref[rows, :] = user_grad(error, vt16) + user_grad(far, xt16)
            share += item_grad(own16, error)
        share_ref[...] = share

    return pl.pallas_call(
        body,
        in_specs=[vmem] * 5,
        out_specs=[vmem] * 2,
        out_shape=[
            jax.ShapeDtypeStruct((z.half, z.rank), f32),
            jax.ShapeDtypeStruct((z.rank, z.items), f32),
        ],
        compiler_params=pltpu.CompilerParams(vmem_limit_bytes=24 * 2**20),
        cost_estimate=visit_cost(z, 5),
        name="user_visit",
    )(own, panel, partner_panel, s_own, s_partner)


def panel_visit(z, other, panel, share, s_oth, last):
    def body(oth_ref, m_ref, share_ref, st_ref, mout_ref):
        vt = read_panel(z, m_ref)
        step = read_steps(z, m_ref)
        oth16 = oth_ref[...].astype(bf16)
        grad_t = share_ref[...] + item_grad(oth16, errors(z, oth16, vt.astype(bf16), st_ref))
        vnew = updated(vt, step, grad_t)
        if last:
            for c in range(z.col_tiles):
                cols = slice(c * z.tile, (c + 1) * z.tile)
                mout_ref[c * z.tile : (c + 1) * z.tile, :] = vnew[:, cols].T
        else:
            write_panel(z, mout_ref, vnew, step)

    rows = z.items if last else z.panel_rows
    return pl.pallas_call(
        body,
        in_specs=[vmem] * 4,
        out_specs=vmem,
        out_shape=jax.ShapeDtypeStruct((rows, z.tile), f32),
        compiler_params=pltpu.CompilerParams(vmem_limit_bytes=24 * 2**20),
        cost_estimate=visit_cost(z, 2),
        name="panel_visit",
    )(other, panel, share, s_oth)


def outputs(z, side, own, other, panel):
    def body(side_ref, own_ref, oth_ref, v_ref, u_hbm, v_hbm, sems):
        side = side_ref[0]
        own_at = pl.multiple_of(side * z.half, z.half)
        oth_at = pl.multiple_of((1 - side) * z.half, z.half)
        copies = [
            pltpu.make_async_copy(own_ref, u_hbm.at[pl.ds(own_at, z.half)], sems.at[0]),
            pltpu.make_async_copy(oth_ref, u_hbm.at[pl.ds(oth_at, z.half)], sems.at[1]),
            pltpu.make_async_copy(v_ref, v_hbm, sems.at[2]),
        ]
        for copy in copies:
            copy.start()
        for copy in copies:
            copy.wait()

    return pl.pallas_call(
        body,
        in_specs=[smem, vmem, vmem, vmem],
        out_specs=[hbm, hbm],
        out_shape=[
            jax.ShapeDtypeStruct((z.users, z.rank), f32),
            jax.ShapeDtypeStruct((z.items, z.rank), f32),
        ],
        scratch_shapes=[pltpu.SemaphoreType.DMA((3,))],
        compiler_params=pltpu.CompilerParams(vmem_limit_bytes=8 * 2**20),
        name="outputs",
    )(side, own, other, panel)


def per_device(
    ratings, user_tile, item_tile, tile_count, user_count, item_count, user_factors, item_factors
):
    z = Sizes(ratings, user_factors, item_factors)
    core = lax.axis_index("split") % 2
    side = core.astype(jnp.int32).reshape(1)
    tiles = (user_tile, item_tile, tile_count.reshape(-1))
    ratings, user_factors, item_factors = (
        pltpu.with_memory_space_constraint(x, pltpu.HBM)
        for x in (ratings, user_factors, item_factors)
    )

    item_count = item_count.reshape(-1, z.tile)
    fixed = [pltpu.with_memory_space_constraint(x, pltpu.HBM) for x in (*tiles, item_count)]
    panel, grad, grad_other, own = first_visit(
        z, side, fixed[:3], ratings, user_factors, item_factors, fixed[3]
    )
    for visit_no in range(z.visits):
        last = visit_no == z.visits - 1
        if visit_no == 0:
            grad = grad + swapped(grad_other, "split", 1)
        else:
            partner_panel = swapped(panel, "split", 1)
            own = own + own_step * (grad + crossed - decay_rate * own)
            other = swapped(own, "split", 1)
            grad, share = user_visit(z, own, panel, partner_panel, s_own, s_partner)
        crossed = swapped(grad, "split", 2)
        if visit_no > 0:
            panel = panel_visit(z, other, panel, share, s_oth, last)
        panel = from_ahead(panel, "blk", 1 - z.visits if last else 1)
        if not last:
            if visit_no == 0:
                s_own, s_oth, own_step = pair_sums(
                    z, 1, side, tiles, ratings, grad, user_count, lax.axis_size("split")
                )
            else:
                s_own, s_oth = pair_sums(z, visit_no + 1, side, tiles, ratings, grad)
            s_partner = swapped(s_oth, "split", 1)
    own = own + own_step * (grad + crossed - decay_rate * own)
    other = swapped(own, "split", 1)
    return outputs(z, side, own, other, panel)


def solution(mesh):
    return jax.shard_map(
        per_device,
        mesh=mesh,
        in_specs=(
            P("blk", None, "split", None, None, None),
            P("blk", None, "split", None),
            P("blk", None, "split", None),
            P("blk", None, "split"),
            P("blk"),
            P(("blk", "split")),
            P("blk", None),
            P(("blk", "split"), None),
        ),
        out_specs=(P("blk", None), P(("blk", "split"), None)),
        check_vma=False,
    )
```
